32 devices in a mesh: grp: 2 (over y), bank: 4 (over z), seg: 4 (over x, core).
Axes of the slice: x: 2, y: 2, z: 4, core: 2. Of those that a mesh axis runs over, the one named last changes fastest.
Arguments:
- strain: bfloat16 [32, 2, 32768], P(('grp', 'seg'), None, 'bank'), parts along dimension 0, may hold values from -6 to 6
- templates: bfloat16 [4, 2, 32768], P('bank'), may hold values from -6 to 6
- length_bins: int32 [4], P('bank'), may hold values from 0 to 3
Outputs:
- snr_table: float32 [4, 32], P('bank', ('grp', 'seg')), parts along dimension 1
- segment_peak: float32 [32], P(('grp', 'seg')), parts along dimension 0
- template_peak: float32 [8], P(('grp', 'bank')), parts along dimension 0
The draws below stay inside these ranges and needn't reach their ends.
There are 2 independent parts, one for each index of `grp`. The reference program is written for one: setup_inputs(seed, part) draws one part's arguments, and reference() takes and returns one part's arrays. A program takes and returns all parts, laid end to end along the dimension named above; an argument that names none is the same for every part. Nothing has to cross between parts.
All inputs are finite; a program needn't handle non-finite values.
Results may differ from the reference program's by a relative error of at most 0.0003.
Values may be sent and summed in bfloat16 or wider, within the bound.
A program may use at most 64 MiB of HBM per device.

```python
import jax
import jax.numpy as jnp
from jax import lax

LEN = 32768
TEMPLATES = 4
SEGMENTS = 16


def with_ends(result, stream_key, least, largest):
    longest = result.shape.index(max(result.shape))
    spots = []
    for shift in (0, 1):
        where = [jax.random.randint(jax.random.fold_in(stream_key, axis), (), 0, length) for axis, length in enumerate(result.shape)]
        where[longest] = (where[longest] + shift) % result.shape[longest]
        spots.append(tuple(where))
    return result.at[spots[0]].set(least).at[spots[1]].set(largest)


def block_scale(rng, shape, pieces, low, largest):
    level, own = 1.0, jax.random.fold_in(rng, 6)
    for axis_at, blocks in pieces:
        draws = jnp.exp(jax.random.uniform(jax.random.fold_in(own, axis_at), (blocks,), jnp.float32, low / len(pieces), largest / len(pieces)))
        level = level * jnp.repeat(draws, shape[axis_at] // blocks).reshape([-1 if axis == axis_at else 1 for axis in range(len(shape))])
    return level


def noise(stream_key, extent, scale, most, split=(), kind=jnp.bfloat16):
    entries = jax.random.normal(stream_key, extent, jnp.float32) * scale
    if len(split) > 0:
        entries = block_scale(stream_key, extent, split, -0.22, 0.18) * entries
    return jnp.clip(entries, min=-most, max=most).astype(kind)


def setup_inputs(seed: int = 0, part: int = 0) -> dict:
    splits = jax.random.split(jax.random.key(seed), 4)
    part_keys = jax.random.split(jax.random.fold_in(splits[3], part), 4)
    strain = noise(part_keys[0], (SEGMENTS, 2, LEN), 1.0, 6.0, ((0, 4), (2, 4)))
    templates = noise(splits[1], (TEMPLATES, 2, LEN), 1.0, 6.0, ((0, 4),))
    length_bins = with_ends(jax.random.randint(splits[2], (TEMPLATES,), 0, 4), jax.random.fold_in(splits[2], 1), 0, 3).astype(jnp.int32)
    return {"strain": strain, "templates": templates, "length_bins": length_bins}


EPSILON = 1e-06

def reference(strain, templates, length_bins):
    seg_real = strain[:, 0, :].astype(jnp.float32)
    seg_imag = strain[:, 1, :].astype(jnp.float32)
    positions = jnp.arange(LEN, dtype=jnp.int32)

    def one_template(inputs):
        template, length_bin = inputs
        cutoff = jnp.right_shift(jnp.int32(LEN), length_bin.astype(jnp.int32))
        keep_mask = positions < cutoff
        tpl_real = jnp.where(keep_mask, template[0].astype(jnp.float32), 0.0)
        tpl_imag = jnp.where(keep_mask, template[1].astype(jnp.float32), 0.0)
        norm_value = jnp.sqrt(jnp.sum(tpl_real * tpl_real + tpl_imag * tpl_imag) + EPSILON)
        prod_real = tpl_real * seg_real + tpl_imag * seg_imag
        prod_imag = tpl_real * seg_imag - tpl_imag * seg_real
        series = jnp.fft.ifft(prod_real + 1j * prod_imag, axis=-1) * LEN
        peak_power = lax.optimization_barrier(jnp.max(jnp.real(series) ** 2 + jnp.imag(series) ** 2, axis=-1))
        return jnp.sqrt(peak_power) / norm_value
    snr_table = lax.map(one_template, (templates, length_bins))
    return (snr_table, lax.optimization_barrier(jnp.max(snr_table, axis=0)), lax.optimization_barrier(jnp.max(snr_table, axis=1)))
```

```python
import functools
import math

import jax
import jax.numpy as jnp
import numpy as np
from jax import lax
from jax.experimental import pallas as pl
from jax.experimental.pallas import tpu as pltpu
from jax.sharding import PartitionSpec as P

MESH = pl.DeviceIdType.MESH
EPSILON = 1e-06
LANES = 128


def split(value):
    high = value.astype(jnp.bfloat16)
    low = (value - high.astype(jnp.float32)).astype(jnp.bfloat16)
    return high, low


def tables(length):
    rows = length // LANES
    half = rows // 2

    def root(phase, period):
        angle = 2.0 * math.pi * (phase % period) / period
        return np.cos(angle), np.sin(angle)

    r = np.arange(half)
    c = np.arange(LANES)
    row_c, row_s = root(np.outer(r, r), half)
    first = np.block([[row_c, -row_s], [row_s, row_c]])
    col_c, col_s = root(np.outer(c, c), LANES)
    last = np.block([[col_c, col_s], [-col_s, col_c]])
    odd = np.stack([np.broadcast_to(part[:, None], (half, LANES)) for part in root(r, rows)])
    turn = [root(np.outer(2 * r + p, c), length) for p in (0, 1)]
    turn = np.stack([np.concatenate([turn[0][i], turn[1][i]], axis=1) for i in (0, 1)])

    def halves(matrix):
        high = matrix.astype(jnp.bfloat16)
        low = (matrix - high.astype(np.float64)).astype(jnp.bfloat16)
        return high, low

    f_high, f_low = halves(first)
    l_high, l_low = halves(last)
    first = np.concatenate([f_high, f_high, f_low], axis=1)
    last = np.concatenate([l_high, l_high, l_low], axis=0)
    return first, last, odd.astype(np.float32), turn.astype(np.float32)


def kernel(
    banks, segs, chunks,
    strain_ref, tpl_ref, bins_ref, first_hbm, last_hbm, odd_hbm, turn_hbm,
    out_ref,
    held, tpl_re, tpl_im, work, first, last, odd, turn, row_bank, row_seg,
    table_sem, right_sem, left_sem, recv_sem, bank_send, bank_recv, seg_send, seg_recv,
):
    me = lax.axis_index("bank")
    my_seg = lax.axis_index("seg")
    count, depth, _ = strain_ref.shape
    size = count // chunks
    rows = tpl_ref.shape[0] // 2
    half = rows // 2

    barrier = pltpu.get_barrier_semaphore()
    has_left, has_right = me > 0, me < banks - 1

    @pl.when(has_left)
    def _():
        pl.semaphore_signal(barrier, inc=1, device_id={"bank": me - 1}, device_id_type=MESH)

    @pl.when(has_right)
    def _():
        pl.semaphore_signal(barrier, inc=1, device_id={"bank": me + 1}, device_id_type=MESH)

    for step in range(1, segs):
        pl.semaphore_signal(
            barrier, inc=1, device_id={"seg": lax.rem(my_seg + step, segs)}, device_id_type=MESH
        )
    loads = [
        pltpu.make_async_copy(source, target, table_sem.at[i])
        for i, (source, target) in enumerate(
            ((first_hbm, first), (odd_hbm, odd), (turn_hbm, turn), (last_hbm, last))
        )
    ]
    for load in loads:
        load.start()
    pl.semaphore_wait(barrier, has_left.astype(jnp.int32) + has_right.astype(jnp.int32) + segs - 1)

    def part(chunk):
        return pl.ds(chunk * size, size)

    def move(source, origin, chunk, step):
        sems = right_sem if step > 0 else left_sem
        return pltpu.make_async_remote_copy(
            src_ref=source,
            dst_ref=held.at[origin, part(chunk)],
            send_sem=sems.at[origin, chunk],
            recv_sem=recv_sem.at[origin, chunk],
            device_id={"bank": me + step},
            device_id_type=MESH,
        )

    for chunk in range(chunks):
        @pl.when(has_right)
        def _():
            move(strain_ref.at[part(chunk)], me, chunk, 1).start()

        @pl.when(has_left)
        def _():
            move(strain_ref.at[part(chunk)], me, chunk, -1).start()

    held[me] = strain_ref[...]

    work[...] = tpl_ref[...].astype(jnp.float32)
    position = lax.broadcasted_iota(jnp.int32, (rows, LANES), 0) * LANES
    position = position + lax.broadcasted_iota(jnp.int32, (rows, LANES), 1)
    keep = position < lax.shift_right_logical(jnp.int32(rows * LANES), bins_ref[0])
    real = jnp.where(keep, work[pl.ds(0, rows, stride=2), :], 0.0)
    imag = jnp.where(keep, work[pl.ds(1, rows, stride=2), :], 0.0)
    tpl_re[...] = real
    tpl_im[...] = imag
    sigma = jnp.sqrt(jnp.sum(real * real + imag * imag, keepdims=True) + EPSILON)

    for load in loads:
        load.wait()

    def peak(seg):
        work[...] = held[:, seg].reshape(2 * rows, LANES).astype(jnp.float32)
        s_re = work[pl.ds(0, rows, stride=2), :]
        s_im = work[pl.ds(1, rows, stride=2), :]
        h_re, h_im = tpl_re[...], tpl_im[...]
        q_re = h_re * s_re + h_im * s_im
        q_im = h_re * s_im - h_im * s_re
        even_re, even_im = q_re[:half] + q_re[half:], q_im[:half] + q_im[half:]
        d_re, d_im = q_re[:half] - q_re[half:], q_im[:half] - q_im[half:]
        odd_re = d_re * odd[0] - d_im * odd[1]
        odd_im = d_re * odd[1] + d_im * odd[0]
        y = jnp.concatenate(
            [
                jnp.concatenate([even_re, odd_re], axis=1),
                jnp.concatenate([even_im, odd_im], axis=1),
            ],
            axis=0,
        )
        high, low = split(y)
        u = jnp.dot(
            first[...],
            jnp.concatenate([high, low, high], axis=0),
            preferred_element_type=jnp.float32,
        )
        u_re, u_im = u[:half], u[half:]
        v_re = u_re * turn[0] - u_im * turn[1]
        v_im = u_re * turn[1] + u_im * turn[0]
        x = jnp.concatenate(
            [
                jnp.concatenate([v_re[:, :LANES], v_im[:, :LANES]], axis=1),
                jnp.concatenate([v_re[:, LANES:], v_im[:, LANES:]], axis=1),
            ],
            axis=0,
        )
        high, low = split(x)
        z = jnp.dot(
            jnp.concatenate([high, low, high], axis=1),
            last[...],
            preferred_element_type=jnp.float32,
        )
        z_re, z_im = z[:, :LANES], z[:, LANES:]
        power = z_re * z_re + z_im * z_im
        return jnp.max(power, keepdims=True)

    lane = lax.broadcasted_iota(jnp.int32, (8, LANES), 1)
    row = jnp.zeros((8, LANES), jnp.float32)
    for distance in range(1, banks):
        for chunk in range(chunks):
            for step in (1, -1):
                origin = me - step * distance
                inside = (origin >= 0) & (origin < banks)

                @pl.when(inside)
                def _():
                    block = held.at[origin, part(chunk)]
                    move(block, origin, chunk, step).wait_recv()

                    @pl.when((me + step >= 0) & (me + step < banks))
                    def _():
                        move(block, origin, chunk, step).start()

            if distance == banks - 1:
                for seg in range(chunk * size, (chunk + 1) * size):
                    row = jnp.where(lane == seg, jnp.sqrt(peak(seg)) / sigma, row)

    row_bank[me] = row
    row_seg[my_seg] = row

    def tell(buffer, axis, index, peer, send, recv):
        return pltpu.make_async_remote_copy(
            src_ref=buffer.at[index],
            dst_ref=buffer.at[index],
            send_sem=send.at[peer],
            recv_sem=recv.at[index],
            device_id={axis: peer},
            device_id_type=MESH,
        )

    groups = (
        (row_bank, "bank", me, banks, bank_send, bank_recv),
        (row_seg, "seg", my_seg, segs, seg_send, seg_recv),
    )
    for buffer, axis, index, number, send, recv in groups:
        for step in range(1, number):
            tell(buffer, axis, index, lax.rem(index + step, number), send, recv).start()
    for chunk in range(chunks):
        for step, sems in ((1, right_sem), (-1, left_sem)):
            for distance in range(banks):
                origin = me - step * distance

                @pl.when((origin >= 0) & (origin < banks) & (me + step >= 0) & (me + step < banks))
                def _():
                    move(held.at[origin, part(chunk)], origin, chunk, step).wait_send()

    for buffer, axis, index, number, send, recv in reversed(groups):
        for step in range(1, number):
            other = lax.rem(index + step, number)
            tell(buffer, axis, other, other, send, recv).wait_recv()
    segment_peak = jnp.max(row_bank[...], axis=0)
    template_peak = jnp.max(row_seg[...], keepdims=True)[0]
    line = lax.broadcasted_iota(jnp.int32, (8, LANES), 0)
    out_ref[...] = jnp.where(line == 0, row, jnp.where(line == 1, segment_peak, template_peak))
    for buffer, axis, index, number, send, recv in groups:
        for step in range(1, number):
            tell(buffer, axis, index, lax.rem(index + step, number), send, recv).wait_send()


def per_device(banks, segs, strain, templates, length_bins):
    count, _, width = strain.shape
    length = templates.shape[2]
    depth, rows = width // LANES, length // LANES
    chunks = count if banks <= 8 else 1
    first, last, odd, turn = tables(length)
    strain = strain.reshape(count, 2, depth, LANES).transpose(0, 2, 1, 3).reshape(count, 2 * depth, LANES)
    tpl = templates.reshape(2, rows, LANES).transpose(1, 0, 2).reshape(2 * rows, LANES)
    vmem = pl.BlockSpec(memory_space=pltpu.VMEM)
    smem = pl.BlockSpec(memory_space=pltpu.SMEM)
    hbm = pl.BlockSpec(memory_space=pl.ANY)
    dma = pltpu.SemaphoreType.DMA
    out = pl.pallas_call(
        functools.partial(kernel, banks, segs, chunks),
        out_shape=jax.ShapeDtypeStruct((8, LANES), jnp.float32),
        in_specs=[vmem, vmem, smem, hbm, hbm, hbm, hbm],
        out_specs=vmem,
        scratch_shapes=[
            pltpu.VMEM((banks, count, 2 * depth, LANES), jnp.bfloat16),
            pltpu.VMEM((rows, LANES), jnp.float32),
            pltpu.VMEM((rows, LANES), jnp.float32),
            pltpu.VMEM((2 * rows, LANES), jnp.float32),
            pltpu.VMEM(first.shape, first.dtype),
            pltpu.VMEM(last.shape, last.dtype),
            pltpu.VMEM(odd.shape, odd.dtype),
            pltpu.VMEM(turn.shape, turn.dtype),
            pltpu.VMEM((banks, 8, LANES), jnp.float32),
            pltpu.VMEM((segs, 8, LANES), jnp.float32),
            dma((4,)),
            dma((banks, chunks)),
            dma((banks, chunks)),
            dma((banks, chunks)),
            dma((banks,)),
            dma((banks,)),
            dma((segs,)),
            dma((segs,)),
        ],
        compiler_params=pltpu.CompilerParams(collective_id=0, has_side_effects=True),
        name="search",
    )(strain, tpl, length_bins, first, last, odd, turn)
    return out[0:1, :count], out[1, :count], out[2, 0:1]


def solution(mesh):
    placed = (P(("grp", "seg"), None, "bank"), P("bank", None, None), P("bank"))
    return jax.shard_map(
        functools.partial(per_device, mesh.shape["bank"], mesh.shape["seg"]),
        mesh=mesh,
        in_specs=placed,
        out_specs=(P("bank", ("grp", "seg")), P(("grp", "seg")), P(("grp", "bank"))),
        check_vma=False,
    )
```

```python
import functools
import math

import jax
import jax.numpy as jnp
import numpy as np
from jax import lax
from jax.experimental import pallas as pl
from jax.experimental.pallas import tpu as pltpu
from jax.sharding import PartitionSpec as P

MESH = pl.DeviceIdType.MESH
EPSILON = 1e-06
LANES = 128


def split(value):
    high = value.astype(jnp.bfloat16)
    low = (value - high.astype(jnp.float32)).astype(jnp.bfloat16)
    return high, low


def tables(length):
    rows = length // LANES
    half = rows // 2

    def root(phase, period):
        angle = 2.0 * math.pi * (phase % period) / period
        return np.cos(angle), np.sin(angle)

    r = np.arange(half)
    c = np.arange(LANES)
    row_c, row_s = root(np.outer(r, r), half)
    first = np.block([[row_c, -row_s], [row_s, row_c]])
    col_c, col_s = root(np.outer(c, c), LANES)
    last = np.block([[col_c, col_s], [-col_s, col_c]])
    odd = np.stack([np.broadcast_to(part[:, None], (half, LANES)) for part in root(r, rows)])
    turn = [root(np.outer(2 * r + p, c), length) for p in (0, 1)]
    turn = np.stack([np.concatenate([turn[0][i], turn[1][i]], axis=1) for i in (0, 1)])

    def halves(matrix):
        high = matrix.astype(jnp.bfloat16)
        low = (matrix - high.astype(np.float64)).astype(jnp.bfloat16)
        return high, low

    f_high, f_low = halves(first)
    l_high, l_low = halves(last)
    first = np.concatenate([f_high, f_high, f_low], axis=1)
    last = np.concatenate([l_high, l_high, l_low], axis=0)
    return first, last, odd.astype(np.float32), turn.astype(np.float32)


def kernel(
    banks, segs, chunks,
    strain_hbm, tpl_hbm, bins_ref, first_hbm, last_hbm, odd_hbm, turn_hbm,
    out_ref,
    strain_ref, tpl_ref, held, tpl_re, tpl_im, work, first, last, odd, turn, row_bank, row_seg,
    input_sem, table_sem, right_sem, left_sem, recv_sem, bank_send, bank_recv, seg_send, seg_recv,
):
    me = lax.axis_index("bank")
    my_seg = lax.axis_index("seg")
    count, depth, _ = strain_ref.shape
    size = count // chunks
    rows = tpl_ref.shape[0] // 2
    half = rows // 2

    def part(chunk):
        return pl.ds(chunk * size, size)

    barrier = pltpu.get_barrier_semaphore()
    has_left, has_right = me > 0, me < banks - 1

    @pl.when(has_left)
    def _():
        pl.semaphore_signal(barrier, inc=1, device_id={"bank": me - 1}, device_id_type=MESH)

    @pl.when(has_right)
    def _():
        pl.semaphore_signal(barrier, inc=1, device_id={"bank": me + 1}, device_id_type=MESH)

    for step in range(1, segs):
        pl.semaphore_signal(
            barrier, inc=1, device_id={"seg": lax.rem(my_seg + step, segs)}, device_id_type=MESH
        )
    inputs = [
        pltpu.make_async_copy(source, target, input_sem.at[i])
        for i, (source, target) in enumerate(
            [(strain_hbm.at[part(chunk)], strain_ref.at[part(chunk)]) for chunk in range(chunks)]
            + [(tpl_hbm, tpl_ref)]
        )
    ]
    for load in inputs:
        load.start()
    loads = [
        pltpu.make_async_copy(source, target, table_sem.at[i])
        for i, (source, target) in enumerate(
            ((first_hbm, first), (odd_hbm, odd), (turn_hbm, turn), (last_hbm, last))
        )
    ]
    for load in loads:
        load.start()
    pl.semaphore_wait(barrier, has_left.astype(jnp.int32) + has_right.astype(jnp.int32) + segs - 1)

    def move(source, origin, chunk, step):
        sems = right_sem if step > 0 else left_sem
        return pltpu.make_async_remote_copy(
            src_ref=source,
            dst_ref=held.at[origin, part(chunk)],
            send_sem=sems.at[origin, chunk],
            recv_sem=recv_sem.at[origin, chunk],
            device_id={"bank": me + step},
            device_id_type=MESH,
        )

    for chunk in range(chunks):
        inputs[chunk].wait()

        @pl.when(has_right)
        def _():
            move(strain_ref.at[part(chunk)], me, chunk, 1).start()

        @pl.when(has_left)
        def _():
            move(strain_ref.at[part(chunk)], me, chunk, -1).start()

    held[me] = strain_ref[...]

    for load in inputs[chunks:]:
        load.wait()
    work[...] = tpl_ref[...].astype(jnp.float32)
    position = lax.broadcasted_iota(jnp.int32, (rows, LANES), 0) * LANES
    position = position + lax.broadcasted_iota(jnp.int32, (rows, LANES), 1)
    keep = position < lax.shift_right_logical(jnp.full((1, 1), rows * LANES, jnp.int32), bins_ref[...])
    real = jnp.where(keep, work[pl.ds(0, rows, stride=2), :], 0.0)
    imag = jnp.where(keep, work[pl.ds(1, rows, stride=2), :], 0.0)
    tpl_re[...] = real
    tpl_im[...] = imag
    sigma = jnp.sqrt(jnp.sum(real * real + imag * imag, keepdims=True) + EPSILON)

    for load in loads:
        load.wait()

    def peak(seg):
        work[...] = held[:, seg].reshape(2 * rows, LANES).astype(jnp.float32)
        s_re = work[pl.ds(0, rows, stride=2), :]
        s_im = work[pl.ds(1, rows, stride=2), :]
        h_re, h_im = tpl_re[...], tpl_im[...]
        q_re = h_re * s_re + h_im * s_im
        q_im = h_re * s_im - h_im * s_re
        even_re, even_im = q_re[:half] + q_re[half:], q_im[:half] + q_im[half:]
        d_re, d_im = q_re[:half] - q_re[half:], q_im[:half] - q_im[half:]
        odd_re = d_re * odd[0] - d_im * odd[1]
        odd_im = d_re * odd[1] + d_im * odd[0]
        y = jnp.concatenate(
            [
                jnp.concatenate([even_re, odd_re], axis=1),
                jnp.concatenate([even_im, odd_im], axis=1),
            ],
            axis=0,
        )
        high, low = split(y)
        u = jnp.dot(
            first[...],
            jnp.concatenate([high, low, high], axis=0),
            preferred_element_type=jnp.float32,
        )
        u_re, u_im = u[:half], u[half:]
        v_re = u_re * turn[0] - u_im * turn[1]
        v_im = u_re * turn[1] + u_im * turn[0]
        x = jnp.concatenate(
            [
                jnp.concatenate([v_re[:, :LANES], v_im[:, :LANES]], axis=1),
                jnp.concatenate([v_re[:, LANES:], v_im[:, LANES:]], axis=1),
            ],
            axis=0,
        )
        high, low = split(x)
        z = jnp.dot(
            jnp.concatenate([high, low, high], axis=1),
            last[...],
            preferred_element_type=jnp.float32,
        )
        z_re, z_im = z[:, :LANES], z[:, LANES:]
        power = z_re * z_re + z_im * z_im
        return jnp.max(power, keepdims=True)

    lane = lax.broadcasted_iota(jnp.int32, (8, LANES), 1)
    row = jnp.zeros((8, LANES), jnp.float32)
    for distance in range(1, banks):
        for chunk in range(chunks):
            for step in (1, -1):
                origin = me - step * distance
                inside = (origin >= 0) & (origin < banks)

                @pl.when(inside)
                def _():
                    block = held.at[origin, part(chunk)]
                    move(block, origin, chunk, step).wait_recv()

                    @pl.when((me + step >= 0) & (me + step < banks))
                    def _():
                        move(block, origin, chunk, step).start()

            if distance == banks - 1:
                for seg in range(chunk * size, (chunk + 1) * size):
                    row = jnp.where(lane == seg, jnp.sqrt(peak(seg)) / sigma, row)

    row_bank[me] = row
    row_seg[my_seg] = row

    def tell(buffer, axis, index, peer, send, recv):
        return pltpu.make_async_remote_copy(
            src_ref=buffer.at[index],
            dst_ref=buffer.at[index],
            send_sem=send.at[peer],
            recv_sem=recv.at[index],
            device_id={axis: peer},
            device_id_type=MESH,
        )

    groups = (
        (row_bank, "bank", me, banks, bank_send, bank_recv),
        (row_seg, "seg", my_seg, segs, seg_send, seg_recv),
    )
    for buffer, axis, index, number, send, recv in groups:
        for step in range(1, number):
            tell(buffer, axis, index, lax.rem(index + step, number), send, recv).start()
    for chunk in range(chunks):
        for step, sems in ((1, right_sem), (-1, left_sem)):
            for distance in range(banks):
                origin = me - step * distance

                @pl.when((origin >= 0) & (origin < banks) & (me + step >= 0) & (me + step < banks))
                def _():
                    move(held.at[origin, part(chunk)], origin, chunk, step).wait_send()

    for buffer, axis, index, number, send, recv in reversed(groups):
        for step in range(1, number):
            other = lax.rem(index + step, number)
            tell(buffer, axis, other, other, send, recv).wait_recv()
    segment_peak = jnp.max(row_bank[...], axis=0)
    template_peak = jnp.max(row_seg[...], keepdims=True)[0]
    line = lax.broadcasted_iota(jnp.int32, (8, LANES), 0)
    out_ref[...] = jnp.where(line == 0, row, jnp.where(line == 1, segment_peak, template_peak))
    for buffer, axis, index, number, send, recv in groups:
        for step in range(1, number):
            tell(buffer, axis, index, lax.rem(index + step, number), send, recv).wait_send()


def unpack(out_ref, table_ref, segment_ref, template_ref):
    table_ref[...] = out_ref[0:1, : table_ref.shape[1]]
    segment_ref[...] = out_ref[1, : segment_ref.shape[0]]
    template_ref[...] = out_ref[2, :1]


def per_device(banks, segs, strain, templates, length_bins):
    count, _, width = strain.shape
    length = templates.shape[2]
    depth, rows = width // LANES, length // LANES
    chunks = count if banks <= 8 else 1
    first, last, odd, turn = tables(length)
    strain = strain.reshape(count, 2, depth, LANES).transpose(0, 2, 1, 3).reshape(count, 2 * depth, LANES)
    tpl = templates.reshape(2, rows, LANES).transpose(1, 0, 2).reshape(2 * rows, LANES)
    vmem = pl.BlockSpec(memory_space=pltpu.VMEM)
    hbm = pl.BlockSpec(memory_space=pltpu.HBM)
    dma = pltpu.SemaphoreType.DMA
    out = pl.pallas_call(
        functools.partial(kernel, banks, segs, chunks),
        out_shape=jax.ShapeDtypeStruct((8, LANES), jnp.float32),
        in_specs=[hbm, hbm, vmem, hbm, hbm, hbm, hbm],
        out_specs=vmem,
        scratch_shapes=[
            pltpu.VMEM(strain.shape, strain.dtype),
            pltpu.VMEM(tpl.shape, tpl.dtype),
            pltpu.VMEM((banks, count, 2 * depth, LANES), jnp.bfloat16),
            pltpu.VMEM((rows, LANES), jnp.float32),
            pltpu.VMEM((rows, LANES), jnp.float32),
            pltpu.VMEM((2 * rows, LANES), jnp.float32),
            pltpu.VMEM(first.shape, first.dtype),
            pltpu.VMEM(last.shape, last.dtype),
            pltpu.VMEM(odd.shape, odd.dtype),
            pltpu.VMEM(turn.shape, turn.dtype),
            pltpu.VMEM((banks, 8, LANES), jnp.float32),
            pltpu.VMEM((segs, 8, LANES), jnp.float32),
            dma((chunks + 1,)),
            dma((4,)),
            dma((banks, chunks)),
            dma((banks, chunks)),
            dma((banks, chunks)),
            dma((banks,)),
            dma((banks,)),
            dma((segs,)),
            dma((segs,)),
        ],
        compiler_params=pltpu.CompilerParams(collective_id=0, has_side_effects=True),
        name="search",
    )(strain, tpl, length_bins.reshape(1, 1), first, last, odd, turn)
    return pl.pallas_call(
        unpack,
        out_shape=[
            jax.ShapeDtypeStruct((1, count), jnp.float32),
            jax.ShapeDtypeStruct((count,), jnp.float32),
            jax.ShapeDtypeStruct((1,), jnp.float32),
        ],
        in_specs=[vmem],
        out_specs=[vmem] * 3,
        name="unpack",
    )(out)


def solution(mesh):
    placed = (P(("grp", "seg"), None, "bank"), P("bank", None, None), P("bank"))
    return jax.shard_map(
        functools.partial(per_device, mesh.shape["bank"], mesh.shape["seg"]),
        mesh=mesh,
        in_specs=placed,
        out_specs=(P("bank", ("grp", "seg")), P(("grp", "seg")), P(("grp", "bank"))),
        check_vma=False,
    )
```

```python
import functools
import math

import jax
import jax.numpy as jnp
import numpy as np
from jax import lax
from jax.experimental import pallas as pl
from jax.experimental.pallas import tpu as pltpu
from jax.sharding import PartitionSpec as P

MESH = pl.DeviceIdType.MESH
EPSILON = 1e-06
LANES = 128


def split(value):
    high = value.astype(jnp.bfloat16)
    low = (value - high.astype(jnp.float32)).astype(jnp.bfloat16)
    return high, low


def tables(length):
    rows = length // LANES
    half = rows // 2

    def root(phase, period):
        angle = 2.0 * math.pi * (phase % period) / period
        return np.cos(angle), np.sin(angle)

    r = np.arange(half)
    c = np.arange(LANES)
    row_c, row_s = root(np.outer(r, r), half)
    first = np.block([[row_c, -row_s], [row_s, row_c]])
    col_c, col_s = root(np.outer(c, c), LANES)
    last = np.block([[col_c, col_s], [-col_s, col_c]])
    odd = np.stack([np.broadcast_to(part[:, None], (half, LANES)) for part in root(r, rows)])
    turn = [root(np.outer(2 * r + p, c), length) for p in (0, 1)]
    turn = np.stack([np.concatenate([turn[0][i], turn[1][i]], axis=1) for i in (0, 1)])

    def halves(matrix):
        high = matrix.astype(jnp.bfloat16)
        low = (matrix - high.astype(np.float64)).astype(jnp.bfloat16)
        return high, low

    f_high, f_low = halves(first)
    l_high, l_low = halves(last)
    first = np.concatenate([f_high, f_high, f_low], axis=1)
    last = np.concatenate([l_high, l_high, l_low], axis=0)
    return first, last, odd.astype(np.float32), turn.astype(np.float32)


def kernel(
    banks, segs, chunks, give,
    strain_hbm, tpl_hbm, bins_ref, first_hbm, last_hbm, odd_hbm, turn_hbm,
    out_ref,
    strain_ref, tpl_ref, masked, lent, held, tpl_re, tpl_im, two_re, two_im, work, first, last, odd, turn,
    row_bank, row_seg, row_far,
    input_sem, table_sem, right_sem, left_sem, recv_sem, bank_send, bank_recv, seg_send, seg_recv,
    far_send, far_recv, tpl_send, tpl_recv,
):
    me = lax.axis_index("bank")
    my_seg = lax.axis_index("seg")
    count, depth, _ = strain_ref.shape
    size = count // chunks
    rows = tpl_ref.shape[0] // 2
    half = rows // 2

    def part(chunk):
        return pl.ds(chunk * size, size)

    barrier = pltpu.get_barrier_semaphore()
    has_left, has_right = me > 0, me < banks - 1
    is_end = jnp.logical_not(has_left & has_right) & (give > 0)
    helps = ((me == 1) | (me == banks - 2)) & (give > 0)
    helper = jnp.where(me == 0, 1, banks - 2)
    helped = jnp.where(me == 1, 0, banks - 1)

    def wanted(device, chunk):
        least = 1 if chunk >= chunks - give else 0
        return (device >= least) & (device < banks - least)


    @pl.when(has_left)
    def _():
        pl.semaphore_signal(barrier, inc=1, device_id={"bank": me - 1}, device_id_type=MESH)

    @pl.when(has_right)
    def _():
        pl.semaphore_signal(barrier, inc=1, device_id={"bank": me + 1}, device_id_type=MESH)

    for step in range(1, segs):
        pl.semaphore_signal(
            barrier, inc=1, device_id={"seg": lax.rem(my_seg + step, segs)}, device_id_type=MESH
        )
    if give:
        for step in range(1, segs):
            @pl.when(is_end)
            def _():
                pl.semaphore_signal(
                    barrier, inc=1, device_id={"bank": helper, "seg": lax.rem(my_seg + step, segs)},
                    device_id_type=MESH,
                )

    inputs = [
        pltpu.make_async_copy(source, target, input_sem.at[i])
        for i, (source, target) in enumerate(
            [(strain_hbm.at[part(chunk)], strain_ref.at[part(chunk)]) for chunk in range(chunks)]
            + [(tpl_hbm, tpl_ref)]
        )
    ]
    for load in inputs:
        load.start()
    loads = [
        pltpu.make_async_copy(source, target, table_sem.at[i])
        for i, (source, target) in enumerate(
            ((first_hbm, first), (odd_hbm, odd), (turn_hbm, turn), (last_hbm, last))
        )
    ]
    for load in loads:
        load.start()
    pl.semaphore_wait(barrier, has_left.astype(jnp.int32) + has_right.astype(jnp.int32) + segs - 1 + helps.astype(jnp.int32) * (segs - 1))

    def move(source, origin, chunk, step):
        sems = right_sem if step > 0 else left_sem
        return pltpu.make_async_remote_copy(
            src_ref=source,
            dst_ref=held.at[origin, part(chunk)],
            send_sem=sems.at[origin, chunk],
            recv_sem=recv_sem.at[origin, chunk],
            device_id={"bank": me + step},
            device_id_type=MESH,
        )

    for chunk in range(chunks):
        inputs[chunk].wait()

        @pl.when(wanted(me + 1, chunk))
        def _():
            move(strain_ref.at[part(chunk)], me, chunk, 1).start()

        @pl.when(wanted(me - 1, chunk))
        def _():
            move(strain_ref.at[part(chunk)], me, chunk, -1).start()

    held[me] = strain_ref[...]

    for load in inputs[chunks:]:
        load.wait()
    position = lax.broadcasted_iota(jnp.int32, (2 * rows, LANES), 0) // 2 * LANES
    position = position + lax.broadcasted_iota(jnp.int32, (2 * rows, LANES), 1)
    keep = position < lax.shift_right_logical(jnp.full((1, 1), rows * LANES, jnp.int32), bins_ref[...])
    value = jnp.where(keep, tpl_ref[...].astype(jnp.float32), 0.0)
    if give:
        masked[...] = value.astype(jnp.bfloat16)

    def prepare(interleaved, re_ref, im_ref):
        work[...] = interleaved
        re_ref[...] = work[pl.ds(0, rows, stride=2), :]
        im_ref[...] = work[pl.ds(1, rows, stride=2), :]
        return jnp.sqrt(jnp.sum(interleaved * interleaved, keepdims=True) + EPSILON)

    sigma = prepare(value, tpl_re, tpl_im)

    def lend():
        return pltpu.make_async_remote_copy(
            src_ref=masked, dst_ref=lent, send_sem=tpl_send.at[0], recv_sem=tpl_recv.at[0],
            device_id={"bank": helper}, device_id_type=MESH,
        )

    if give:
        @pl.when(is_end)
        def _():
            lend().start()

    for load in loads:
        load.wait()

    def peak(seg, re_ref, im_ref):
        work[...] = held[:, seg].reshape(2 * rows, LANES).astype(jnp.float32)
        s_re = work[pl.ds(0, rows, stride=2), :]
        s_im = work[pl.ds(1, rows, stride=2), :]
        h_re, h_im = re_ref[...], im_ref[...]
        q_re = h_re * s_re + h_im * s_im
        q_im = h_re * s_im - h_im * s_re
        even_re, even_im = q_re[:half] + q_re[half:], q_im[:half] + q_im[half:]
        d_re, d_im = q_re[:half] - q_re[half:], q_im[:half] - q_im[half:]
        odd_re = d_re * odd[0] - d_im * odd[1]
        odd_im = d_re * odd[1] + d_im * odd[0]
        y = jnp.concatenate(
            [
                jnp.concatenate([even_re, odd_re], axis=1),
                jnp.concatenate([even_im, odd_im], axis=1),
            ],
            axis=0,
        )
        high, low = split(y)
        u = jnp.dot(
            first[...],
            jnp.concatenate([high, low, high], axis=0),
            preferred_element_type=jnp.float32,
        )
        u_re, u_im = u[:half], u[half:]
        v_re = u_re * turn[0] - u_im * turn[1]
        v_im = u_re * turn[1] + u_im * turn[0]
        x = jnp.concatenate(
            [
                jnp.concatenate([v_re[:, :LANES], v_im[:, :LANES]], axis=1),
                jnp.concatenate([v_re[:, LANES:], v_im[:, LANES:]], axis=1),
            ],
            axis=0,
        )
        high, low = split(x)
        z = jnp.dot(
            jnp.concatenate([high, low, high], axis=1),
            last[...],
            preferred_element_type=jnp.float32,
        )
        z_re, z_im = z[:, :LANES], z[:, LANES:]
        power = z_re * z_re + z_im * z_im
        return jnp.max(power, keepdims=True)

    lane = lax.broadcasted_iota(jnp.int32, (8, LANES), 1)
    line = lax.broadcasted_iota(jnp.int32, (8, LANES), 0)
    row_bank[me] = jnp.zeros((8, LANES), jnp.float32)

    def note(seg, which, snr):
        row_bank[me] = jnp.where((lane == seg) & (line == which), snr, row_bank[me])

    for distance in range(1, banks):
        for chunk in range(chunks):
            for step in (1, -1):
                origin = me - step * distance
                inside = (origin >= 0) & (origin < banks) & wanted(me, chunk)

                @pl.when(inside)
                def _():
                    block = held.at[origin, part(chunk)]
                    move(block, origin, chunk, step).wait_recv()

                    @pl.when(wanted(me + step, chunk))
                    def _():
                        move(block, origin, chunk, step).start()

            if distance == banks - 1:
                for seg in range(chunk * size, (chunk + 1) * size):
                    if chunk < chunks - give:
                        note(seg, 0, jnp.sqrt(peak(seg, tpl_re, tpl_im)) / sigma)
                        continue

                    @pl.when(helps)
                    def _():
                        if chunk == chunks - give:
                            lend().wait_recv()
                        sigma_two = prepare(lent[...].astype(jnp.float32), two_re, two_im)
                        one = peak(seg, tpl_re, tpl_im)
                        two = peak(seg, two_re, two_im)
                        note(seg, 0, jnp.sqrt(one) / sigma)
                        note(seg, 1, jnp.sqrt(two) / sigma_two)

    row_seg[my_seg] = row_bank[me]

    def tell(buffer, axis, index, peer, send, recv):
        return pltpu.make_async_remote_copy(
            src_ref=buffer.at[index],
            dst_ref=buffer.at[index],
            send_sem=send.at[peer],
            recv_sem=recv.at[index],
            device_id={axis: peer},
            device_id_type=MESH,
        )

    def far(peer):
        return pltpu.make_async_remote_copy(
            src_ref=row_seg.at[my_seg], dst_ref=row_far.at[my_seg],
            send_sem=far_send.at[peer], recv_sem=far_recv.at[my_seg],
            device_id={"bank": helped, "seg": peer}, device_id_type=MESH,
        )

    def heard(peer):
        return pltpu.make_async_remote_copy(
            src_ref=row_seg.at[my_seg], dst_ref=row_far.at[peer],
            send_sem=far_send.at[peer], recv_sem=far_recv.at[peer],
            device_id={"bank": helper, "seg": peer}, device_id_type=MESH,
        )

    groups = (
        (row_bank, "bank", me, banks, bank_send, bank_recv),
        (row_seg, "seg", my_seg, segs, seg_send, seg_recv),
    )
    for buffer, axis, index, number, send, recv in groups:
        for step in range(1, number):
            tell(buffer, axis, index, lax.rem(index + step, number), send, recv).start()
    peers = [lax.rem(my_seg + step, segs) for step in range(1, segs)]
    if give:
        @pl.when(helps)
        def _():
            for peer in peers:
                far(peer).start()
    for chunk in range(chunks):
        for step, sems in ((1, right_sem), (-1, left_sem)):
            for distance in range(banks):
                origin = me - step * distance

                @pl.when((origin >= 0) & (origin < banks) & wanted(me + step, chunk))
                def _():
                    move(held.at[origin, part(chunk)], origin, chunk, step).wait_send()

    for buffer, axis, index, number, send, recv in reversed(groups):
        for step in range(1, number):
            other = lax.rem(index + step, number)
            tell(buffer, axis, other, other, send, recv).wait_recv()
    segment_peak = jnp.max(row_bank[...], axis=(0, 1))[None, :]
    table = row_bank[me][:1]
    template_row = jnp.max(row_seg[...], axis=0)[:1]

    def give_out(table, template_row):
        template_peak = jnp.max(template_row, axis=1, keepdims=True)
        out_ref[...] = jnp.where(line == 0, table, jnp.where(line == 1, segment_peak, template_peak))

    if give:
        @pl.when(is_end)
        def _():
            theirs = row_bank[helper][1:2]
            every = jnp.maximum(template_row, theirs)
            for peer in peers:
                heard(peer).wait_recv()
                every = jnp.maximum(every, row_far[peer][1:2])
            give_out(jnp.maximum(table, theirs), every)

        @pl.when(jnp.logical_not(is_end))
        def _():
            give_out(table, template_row)

        @pl.when(is_end)
        def _():
            lend().wait_send()

        @pl.when(helps)
        def _():
            for peer in peers:
                far(peer).wait_send()
    else:
        give_out(table, template_row)
    for buffer, axis, index, number, send, recv in groups:
        for step in range(1, number):
            tell(buffer, axis, index, lax.rem(index + step, number), send, recv).wait_send()


def unpack(out_ref, table_ref, segment_ref, template_ref):
    table_ref[...] = out_ref[0:1, : table_ref.shape[1]]
    segment_ref[...] = out_ref[1, : segment_ref.shape[0]]
    template_ref[...] = out_ref[2, :1]


def per_device(banks, segs, strain, templates, length_bins):
    count, _, width = strain.shape
    length = templates.shape[2]
    depth, rows = width // LANES, length // LANES
    chunks = count if banks <= 8 else 1
    give = 1 if banks == 4 and chunks == count > 1 else 0
    first, last, odd, turn = tables(length)
    strain = strain.reshape(count, 2, depth, LANES).transpose(0, 2, 1, 3).reshape(count, 2 * depth, LANES)
    tpl = templates.reshape(2, rows, LANES).transpose(1, 0, 2).reshape(2 * rows, LANES)
    vmem = pl.BlockSpec(memory_space=pltpu.VMEM)
    hbm = pl.BlockSpec(memory_space=pltpu.HBM)
    dma = pltpu.SemaphoreType.DMA
    out = pl.pallas_call(
        functools.partial(kernel, banks, segs, chunks, give),
        out_shape=jax.ShapeDtypeStruct((8, LANES), jnp.float32),
        in_specs=[hbm, hbm, vmem, hbm, hbm, hbm, hbm],
        out_specs=vmem,
        scratch_shapes=[
            pltpu.VMEM(strain.shape, strain.dtype),
            pltpu.VMEM(tpl.shape, tpl.dtype),
            pltpu.VMEM(tpl.shape, tpl.dtype),
            pltpu.VMEM(tpl.shape, tpl.dtype),
            pltpu.VMEM((banks, count, 2 * depth, LANES), jnp.bfloat16),
            pltpu.VMEM((rows, LANES), jnp.float32),
            pltpu.VMEM((rows, LANES), jnp.float32),
            pltpu.VMEM((rows, LANES), jnp.float32),
            pltpu.VMEM((rows, LANES), jnp.float32),
            pltpu.VMEM((2 * rows, LANES), jnp.float32),
            pltpu.VMEM(first.shape, first.dtype),
            pltpu.VMEM(last.shape, last.dtype),
            pltpu.VMEM(odd.shape, odd.dtype),
            pltpu.VMEM(turn.shape, turn.dtype),
            pltpu.VMEM((banks, 8, LANES), jnp.float32),
            pltpu.VMEM((segs, 8, LANES), jnp.float32),
            pltpu.VMEM((segs, 8, LANES), jnp.float32),
            dma((chunks + 1,)),
            dma((4,)),
            dma((banks, chunks)),
            dma((banks, chunks)),
            dma((banks, chunks)),
            dma((banks,)),
            dma((banks,)),
            dma((segs,)),
            dma((segs,)),
            dma((segs,)),
            dma((segs,)),
            dma((1,)),
            dma((1,)),
        ],
        compiler_params=pltpu.CompilerParams(collective_id=0, has_side_effects=True),
        name="search",
    )(strain, tpl, length_bins.reshape(1, 1), first, last, odd, turn)
    return pl.pallas_call(
        unpack,
        out_shape=[
            jax.ShapeDtypeStruct((1, count), jnp.float32),
            jax.ShapeDtypeStruct((count,), jnp.float32),
            jax.ShapeDtypeStruct((1,), jnp.float32),
        ],
        in_specs=[vmem],
        out_specs=[vmem] * 3,
        name="unpack",
    )(out)


def solution(mesh):
    placed = (P(("grp", "seg"), None, "bank"), P("bank", None, None), P("bank"))
    return jax.shard_map(
        functools.partial(per_device, mesh.shape["bank"], mesh.shape["seg"]),
        mesh=mesh,
        in_specs=placed,
        out_specs=(P("bank", ("grp", "seg")), P(("grp", "seg")), P(("grp", "bank"))),
        check_vma=False,
    )
```
